32 devices in a mesh: layer: 8 (over z, y), dp: 4 (over x, core).
Axes of the slice: x: 2, y: 2, z: 4, core: 2. Of those that a mesh axis runs over, the one named last changes fastest.
Arguments:
- states: bfloat16 [8, 1024, 512], P('layer', 'dp'), may hold values from -40 to 40
- guess: bfloat16 [8, 1024, 512], P('layer', 'dp'), may hold values from -6 to 6
- cotangent: bfloat16 [1024, 512], P('dp'), may hold values from -6 to 6
- lengths: int32 [4], P('dp'), may hold values from 128 to 256
- coarse_rate: float32 [8, 512], P('layer'), may hold values from 0.2 to 1
- w_qkv: bfloat16 [8, 512, 1536], P('layer'), may hold values from -0.25 to 0.25
- w_out: bfloat16 [8, 512, 512], P('layer'), may hold values from -0.25 to 0.25
- w_in: bfloat16 [8, 512, 2048], P('layer'), may hold values from -0.25 to 0.25
- w_back: bfloat16 [8, 2048, 512], P('layer'), may hold values from -0.125 to 0.125
- gain_attn: float32 [8, 512], P('layer'), may hold values from 0.5 to 1.5
- gain_ffn: float32 [8, 512], P('layer'), may hold values from 0.5 to 1.5
Outputs:
- adjoint: bfloat16 [8, 1024, 512], P('layer', 'dp')
- coarse_error: float32 [8, 1024, 512], P('layer', 'dp')
- grad_qkv: float32 [8, 512, 1536], P('layer', 'dp')
- grad_out: float32 [8, 512, 512], P('layer', 'dp')
- grad_in: float32 [8, 512, 2048], P('layer', 'dp')
- grad_back: float32 [8, 2048, 512], P('layer', 'dp')
- grad_gain_attn: float32 [8, 512], P('layer', 'dp')
- grad_gain_ffn: float32 [8, 512], P('layer', 'dp')
The draws below stay inside these ranges and needn't reach their ends.
All inputs are finite; a program needn't handle non-finite values.
Results may differ from the reference program's by a relative error of at most 0.028.
The reference program's roundings to bfloat16 on the way count: a program that leaves them out, or rounds other values in their place, can miss the bound.
Values may be sent and summed in bfloat16 or wider, within the bound.
A program may use at most 128 MiB of HBM per device.

```python
import math
import jax
import jax.numpy as jnp
from jax import lax

D = 512
FF = 2048
HEAD_DIM = 64
SEQ = 256
FACTOR = 4
LAYERS = 8
BATCH = 4
TOKENS = 1024


def draw_states(key, part):
    base = jax.random.normal(jax.random.fold_in(key, 11), (LAYERS, TOKENS, D), jnp.float32)
    return jnp.clip(base, -6.0, 6.0).astype(jnp.bfloat16)


def touch_ends(values, key, low, high):
    longest = values.shape.index(max(values.shape))
    spots = []
    for shift in (0, 1):
        where = [jax.random.randint(jax.random.fold_in(key, axis), (), 0, length) for axis, length in enumerate(values.shape)]
        where[longest] = (where[longest] + shift) % values.shape[longest]
        spots.append(tuple(where))
    return values.at[spots[0]].set(low).at[spots[1]].set(high)


def steps_of(key, extent, cuts, low, top_value):
    def one(position, blocks):
        steps = jax.random.uniform(jax.random.fold_in(jax.random.fold_in(key, 6), position), (blocks,), jnp.float32, low / len(cuts), top_value / len(cuts))
        return jnp.repeat(jnp.exp(steps), extent[position] // blocks).reshape((-1,) + (1,) * (len(extent) - position - 1))

    level = one(*cuts[0])
    for cut in cuts[1:]:
        level = level * one(*cut)
    return level


def normal_values(own_key, dims, width, bound, split=(), kind=jnp.bfloat16):
    array = width * jax.random.normal(own_key, dims, jnp.float32)
    if split:
        array = array * steps_of(own_key, dims, split, -0.22, 0.18)
    return jnp.clip(array, -bound, bound).astype(kind)


def setup_inputs(seed: int = 0) -> dict:
    splits = jax.random.split(jax.random.key(seed), 12)
    return {
        "states": draw_states(jax.random.fold_in(splits[11], 71), 0),
        "guess": normal_values(splits[1], (LAYERS, TOKENS, D), 1.0, 6.0, ((0, 8), (1, 4))),
        "cotangent": normal_values(splits[2], (TOKENS, D), 1.0, 6.0, ((0, 4),)),
        "lengths": touch_ends(jax.random.randint(splits[3], (BATCH,), SEQ // 2, SEQ + 1), jax.random.fold_in(splits[3], 1), SEQ // 2, SEQ).astype(jnp.int32),
        "coarse_rate": jnp.clip(jnp.exp(math.log(1.0) - 1.609438 * jax.random.uniform(splits[4], (LAYERS, D), jnp.float32) ** steps_of(splits[4], (LAYERS, D), ((0, 8),), -0.2, 0.2)), 0.2, 1.0),
        "w_qkv": normal_values(splits[5], (LAYERS, D, 3 * D), D ** -0.5, 0.25, ((0, 8),)),
        "w_out": normal_values(splits[6], (LAYERS, D, D), D ** -0.5, 0.25, ((0, 8),)),
        "w_in": normal_values(splits[7], (LAYERS, D, FF), D ** -0.5, 0.25, ((0, 8),)),
        "w_back": normal_values(splits[8], (LAYERS, FF, D), FF ** -0.5, 0.125, ((0, 8),)),
        "gain_attn": jnp.clip(1.0 + 0.1 * jax.random.normal(splits[9], (LAYERS, D), jnp.float32), 0.5, 1.5),
        "gain_ffn": jnp.clip(1.0 + 0.1 * jax.random.normal(splits[10], (LAYERS, D), jnp.float32), 0.5, 1.5),
    }


EPS = 1e-05
DEPTH_GAIN = 6.73
CUBIC = 0.044715
TANH_SCALE = 0.7978845608028654

def batched(form, left, right):
    return jnp.einsum(form, left.astype(jnp.float32), right.astype(jnp.float32), precision=lax.Precision.HIGHEST)

def matmul(left, right):
    return jnp.dot(left, right, preferred_element_type=jnp.float32)

def normalize(row_sum, gain_vec):
    center = row_sum - lax.optimization_barrier(jnp.mean(row_sum, axis=-1, keepdims=True))
    inv_std = lax.rsqrt(lax.optimization_barrier(jnp.mean(center * center, axis=-1, keepdims=True)) + EPS)
    unit_rows = center * inv_std
    return (unit_rows * gain_vec, unit_rows, inv_std)

def norm_back(upstream, unit_rows, inv_std, gain_vec):
    scaled = upstream * gain_vec
    inner_term = scaled - lax.optimization_barrier(jnp.mean(scaled, axis=-1, keepdims=True)) - unit_rows * lax.optimization_barrier(jnp.mean(scaled * unit_rows, axis=-1, keepdims=True))
    return (inv_std * inner_term, lax.optimization_barrier(jnp.sum(upstream * unit_rows, axis=0)))

def forward(state_in, lengths, layer_qkv, layer_out, layer_in, layer_back, gain_one, gain_two):
    tokens = state_in.shape[0]
    model_width = state_in.shape[1]
    sentences = tokens // SEQ
    head_count = model_width // HEAD_DIM
    score_scale = HEAD_DIM ** (-0.5)
    qkv_bf = matmul(state_in, layer_qkv).astype(jnp.bfloat16)
    qkv_heads = qkv_bf.reshape(sentences, SEQ, 3, head_count, HEAD_DIM)
    queries, key_rows, value_rows = (qkv_heads[:, :, 0], qkv_heads[:, :, 1], qkv_heads[:, :, 2])
    positions = jnp.arange(SEQ, dtype=jnp.int32)
    allowed = (positions[None, :] <= positions[:, None])[None, None] & (positions[None, None, None, :] < lengths[:, None, None, None])
    scores = batched('bqhe,bkhe->bhqk', queries, key_rows) * score_scale
    scores = jnp.where(allowed, scores, -1e+30)
    row_max = lax.optimization_barrier(jnp.max(scores, axis=-1, keepdims=True))
    exp_terms = jnp.where(allowed, jnp.exp(scores - row_max), 0.0)
    attn_probs = exp_terms / lax.optimization_barrier(jnp.sum(exp_terms, axis=-1, keepdims=True))
    prob_bf = attn_probs.astype(jnp.bfloat16)
    context = batched('bhqk,bkhe->bqhe', prob_bf, value_rows).astype(jnp.bfloat16).reshape(tokens, model_width)
    first_sum = DEPTH_GAIN * state_in.astype(jnp.float32) + matmul(context, layer_out)
    normed, unit_one, inv_one = normalize(first_sum, gain_one)
    normed_bf = normed.astype(jnp.bfloat16)
    pre_act = matmul(normed_bf, layer_in)
    tanh_part = jnp.tanh(TANH_SCALE * (pre_act + CUBIC * pre_act * pre_act * pre_act))
    hidden = (0.5 * pre_act * (1.0 + tanh_part)).astype(jnp.bfloat16)
    second_sum = DEPTH_GAIN * normed + matmul(hidden, layer_back)
    _, unit_two, inv_two = normalize(second_sum, gain_two)
    return (queries, key_rows, value_rows, attn_probs, prob_bf, context, unit_one, inv_one, normed_bf, pre_act, tanh_part, hidden, unit_two, inv_two)

def backward(upstream, cache, state_in, layer_qkv, layer_out, layer_in, layer_back, gain_one, gain_two):
    queries, key_rows, value_rows, attn_probs, prob_bf, context, unit_one, inv_one, normed_bf, pre_act, tanh_part, hidden, unit_two, inv_two = cache
    tokens = state_in.shape[0]
    model_width = state_in.shape[1]
    score_scale = HEAD_DIM ** (-0.5)
    d_second, grad_two = norm_back(upstream.astype(jnp.float32), unit_two, inv_two, gain_two)
    d_out_bf = d_second.astype(jnp.bfloat16)
    d_hidden = matmul(d_out_bf, layer_back.T)
    deriv = 0.5 * (1.0 + tanh_part) + 0.5 * pre_act * (1.0 - tanh_part * tanh_part) * TANH_SCALE * (1.0 + 3.0 * CUBIC * pre_act * pre_act)
    d_pre_bf = (d_hidden * deriv).astype(jnp.bfloat16)
    d_normed = DEPTH_GAIN * d_second + matmul(d_pre_bf, layer_in.T)
    d_first, grad_one = norm_back(d_normed, unit_one, inv_one, gain_one)
    d_attn_bf = d_first.astype(jnp.bfloat16)
    d_context = matmul(d_attn_bf, layer_out.T).astype(jnp.bfloat16).reshape(queries.shape)
    d_probs = batched('bqhe,bkhe->bhqk', d_context, value_rows)
    d_values = batched('bhqk,bqhe->bkhe', prob_bf, d_context)
    d_scores = attn_probs * (d_probs - lax.optimization_barrier(jnp.sum(attn_probs * d_probs, axis=-1, keepdims=True))) * score_scale
    d_scores_bf = d_scores.astype(jnp.bfloat16)
    d_queries = batched('bhqk,bkhe->bqhe', d_scores_bf, key_rows)
    d_keys = batched('bhqk,bqhe->bkhe', d_scores_bf, queries)
    d_qkv_bf = jnp.stack([d_queries, d_keys, d_values], axis=2).astype(jnp.bfloat16).reshape(tokens, 3 * model_width)
    d_state = (DEPTH_GAIN * d_first + matmul(d_qkv_bf, layer_qkv.T)).astype(jnp.bfloat16)
    factors = (d_qkv_bf, d_attn_bf, d_pre_bf, d_out_bf, normed_bf, hidden, context, grad_one, grad_two)
    return (d_state, factors)

def reference(states, guess, cotangent, lengths, coarse_rate, w_qkv, w_out, w_in, w_back, gain_attn, gain_ffn):
    layer_total = states.shape[0]
    above = jnp.concatenate([guess[1:], cotangent[None]], axis=0)

    def relax_layer(item):
        state_in, upstream, layer_qkv, layer_out, layer_in, layer_back, gain_one, gain_two = item
        cache = forward(state_in, lengths, layer_qkv, layer_out, layer_in, layer_back, gain_one, gain_two)
        return backward(upstream, cache, state_in, layer_qkv, layer_out, layer_in, layer_back, gain_one, gain_two)[0]
    relaxed = lax.map(relax_layer, (states, above, w_qkv, w_out, w_in, w_back, gain_attn, gain_ffn))
    layer_ids = jnp.arange(layer_total, dtype=jnp.int32)
    coarse_mask = (layer_ids % FACTOR == 0) | (layer_ids == layer_total - 1)
    guess_float = guess.astype(jnp.float32)
    residuals = relaxed.astype(jnp.float32) - guess_float
    factor_rows = jnp.where(coarse_mask[:, None], coarse_rate, 1.0)
    offset_rows = jnp.where(coarse_mask[:, None, None], residuals, 0.0)

    def coarse_step(carry, item):
        rate_row, resid_row = item
        coarse_err = rate_row * carry + resid_row
        return (coarse_err, coarse_err)
    _, errors = lax.scan(coarse_step, jnp.zeros(residuals.shape[1:], jnp.float32), (factor_rows, offset_rows), reverse=True)
    corrected = jnp.where(coarse_mask[:, None, None], (guess_float + errors).astype(jnp.bfloat16), relaxed)
    below = jnp.concatenate([corrected[1:], cotangent[None]], axis=0)

    def final_layer(item):
        state_in, upstream, layer_qkv, layer_out, layer_in, layer_back, gain_one, gain_two = item
        cache = forward(state_in, lengths, layer_qkv, layer_out, layer_in, layer_back, gain_one, gain_two)
        d_state, factors = backward(upstream, cache, state_in, layer_qkv, layer_out, layer_in, layer_back, gain_one, gain_two)
        d_qkv_bf, d_attn_bf, d_pre_bf, d_out_bf, normed_bf, hidden, context, grad_one, grad_two = factors
        return (d_state, matmul(state_in.T, d_qkv_bf), matmul(context.T, d_attn_bf), matmul(normed_bf.T, d_pre_bf), matmul(hidden.T, d_out_bf), grad_one, grad_two)
    results = lax.map(final_layer, (states, below, w_qkv, w_out, w_in, w_back, gain_attn, gain_ffn))
    adjoint = jnp.where(coarse_mask[:, None, None], corrected, results[0])
    return (adjoint, errors, results[1], results[2], results[3], results[4], results[5], results[6])
```

```python
import functools

import jax
import jax.numpy as jnp
from jax import lax
from jax.experimental import pallas as pl
from jax.experimental.pallas import tpu as pltpu
from jax.sharding import PartitionSpec as P

HEAD_DIM = 64
SEQ = 256
FACTOR = 4
EPS = 1e-05
DEPTH_GAIN = 6.73
CUBIC = 0.044715
TANH_SCALE = 0.7978845608028654
F32 = jnp.float32
BF = jnp.bfloat16


def nn(a, b):
    return lax.dot_general(a, b, (((1,), (0,)), ((), ())), preferred_element_type=F32)


def nt(a, b):
    return lax.dot_general(a, b, (((1,), (1,)), ((), ())), preferred_element_type=F32)


def tn(a, b):
    return lax.dot_general(a, b, (((0,), (0,)), ((), ())), preferred_element_type=F32)


def mean(v):
    return jnp.mean(v, axis=-1, keepdims=True)


def unit_of(v):
    center = v - mean(v)
    inv = lax.rsqrt(mean(center * center) + EPS)
    return center * inv, inv


def norm_back(up, unit, inv, gain):
    scaled = up * gain
    inner = scaled - mean(scaled) - unit * mean(scaled * unit)
    return inv * inner, jnp.sum(up * unit, axis=0, keepdims=True)


def kernel(
    layers, dpn, coarse,
    len_ref, x_hbm, guess_hbm, cot_hbm, rate_hbm, gain1_hbm, gain2_hbm,
    wqkv_hbm, wout_hbm, win_hbm, wback_hbm,
    adj_ref, err_ref, gqkv_ref, gout_ref, gin_ref, gback_ref, g1_ref, g2_ref,
    x_ref, guess_ref, cot_ref, rate_ref, gain1_ref, gain2_ref,
    wqkv, wout, win, wback,
    qkv, bias, probs, ctx, unit1, unit2, inv1, inv2, normed_bf, hidden, deriv,
    up_bf, dctx, dqkv, dpre, dfirst, relaxed,
    above, above2, crel, cguess, crate, err, err_bf, err_in,
    part_back, part_in, part_out, part_qkv,
    r1_back, r1_in, r1_out, r1_qkv,
    r2_back, r2_in, r2_out, r2_qkv,
    gsum, grecv,
    wsem, lsem, s_up, r_up, s_cg, r_cg, s_cr, r_cr, s_ce, r_ce, s_lz, r_lz,
    s1, q1, s2, q2, s_g, r_g,
):
    layer = lax.axis_index("layer")
    dp = lax.axis_index("dp")
    tokens, width = x_ref.shape
    hidden_units = hidden.shape[1]
    sentences = tokens // SEQ
    pairs = width // 128
    scale = HEAD_DIM ** (-0.5)
    chips = dpn // 2
    chip, core = dp // 2, dp % 2
    last = layers - 1
    is_last = layer == last
    is_coarse = (layer % FACTOR == 0) | is_last
    next_coarse = (((layer + 1) % FACTOR == 0) | (layer + 1 == last)) & (layer < last)
    next_plain = (layer < last) & (((layer + 1) % FACTOR != 0) & (layer + 1 != last))

    def send(src, dst, ssem, rsem, **where):
        return pltpu.make_async_remote_copy(
            src_ref=src, dst_ref=dst, send_sem=ssem, recv_sem=rsem,
            device_id=where, device_id_type=pl.DeviceIdType.MESH,
        )

    loads = [
        pltpu.make_async_copy(a, b, wsem.at[i])
        for i, (a, b) in enumerate(
            ((wqkv_hbm, wqkv), (wout_hbm, wout), (win_hbm, win), (wback_hbm, wback))
        )
    ]
    small = [
        pltpu.make_async_copy(a, b, lsem.at[i])
        for i, (a, b) in enumerate(
            (
                (x_hbm, x_ref), (guess_hbm, guess_ref), (rate_hbm, rate_ref),
                (gain1_hbm, gain1_ref), (gain2_hbm, gain2_ref),
                (cot_hbm, cot_ref),
            )
        )
    ]
    for load in small[:3] + loads[:1] + small[3:] + loads[1:]:
        load.start()

    barrier = pltpu.get_barrier_semaphore()
    for o in range(1, layers):
        pl.semaphore_signal(
            barrier, inc=1, device_id={"layer": lax.rem(layer + o, layers)},
            device_id_type=pl.DeviceIdType.MESH,
        )
    for o in range(1, dpn):
        pl.semaphore_signal(
            barrier, inc=1, device_id={"dp": lax.rem(dp + o, dpn)},
            device_id_type=pl.DeviceIdType.MESH,
        )
    pl.semaphore_wait(barrier, layers - 1 + dpn - 1)

    tops = [(i, c - 1) for i, c in enumerate(coarse)]

    up_guess = lambda: send(
        guess_ref, above, s_up.at[0], r_up.at[0], layer=jnp.maximum(layer - 1, 0)
    )
    up_relaxed = lambda: send(
        relaxed, above2, s_up.at[1], r_up.at[1], layer=jnp.maximum(layer - 1, 0)
    )

    def coarse_sends(src, dst, ssem, rsem, act, own):
        for idx, j in enumerate(coarse):
            reach = [t for i, t in tops if i < idx or (own and i == idx)]
            if reach:

                @pl.when(layer == j)
                def _():
                    for n, t in enumerate(reach[::-1]):
                        act(send(src, dst.at[idx], ssem.at[n], rsem.at[idx], layer=jnp.int32(t)))

    def lazy_sends(act):
        for i, t in tops:
            low = coarse[i - 1] if i else 0

            @pl.when(layer == t)
            def _():
                for n, target in enumerate(range(low, t)):
                    act(send(err_bf, err_in, s_lz.at[n], r_lz.at[0], layer=jnp.int32(target)))

    for load in small[1:3]:
        load.wait()
    pl.when(layer > 0)(lambda: up_guess().start())
    start = lambda c: c.start()
    coarse_sends(rate_ref, crate, s_cr, r_cr, start, True)
    coarse_sends(guess_ref, cguess, s_cg, r_cg, start, False)
    for load in small[:1] + small[3:]:
        load.wait()

    gain1, gain2 = gain1_ref[...], gain2_ref[...]
    loads[0].wait()
    qkv[...] = nn(x_ref[...], wqkv[...]).astype(BF)
    for s in range(sentences):
        rows = pl.ds(s * SEQ, SEQ)
        row_at = lax.broadcasted_iota(jnp.int32, (SEQ, SEQ), 0)
        col_at = lax.broadcasted_iota(jnp.int32, (SEQ, SEQ), 1)
        bias[...] = jnp.where((col_at <= row_at) & (col_at < len_ref[s]), 0.0, -1e30)

        def attend(i, carry):
            lanes = lambda k: pl.ds(pl.multiple_of(k * width + i * 128, 128), 128)
            q, k, v = qkv[rows, lanes(0)], qkv[rows, lanes(1)], qkv[rows, lanes(2)]
            outs = []
            for h in range(2):
                cut = slice(h * HEAD_DIM, (h + 1) * HEAD_DIM)
                sc = nt(q[:, cut], k[:, cut]) * scale + bias[...]
                e = jnp.exp(sc - jnp.max(sc, axis=-1, keepdims=True))
                p = e * (1.0 / jnp.sum(e, axis=-1, keepdims=True))
                probs[s, 2 * i + h] = p
                outs.append(nn(p.astype(BF), v[:, cut]))
            ctx[rows, lanes(0)] = jnp.concatenate(outs, axis=-1).astype(BF)
            return carry

        lax.fori_loop(0, pairs, attend, 0)
    loads[1].wait()
    u, iv = unit_of(DEPTH_GAIN * x_ref[...].astype(F32) + nn(ctx[...], wout[...]))
    unit1[...] = u
    inv1[...] = iv
    normed_bf[...] = (u * gain1).astype(BF)
    loads[2].wait()
    step = 512

    def feed(i, carry):
        lanes = pl.ds(pl.multiple_of(i * step, step), step)
        pre = nn(normed_bf[...], win[:, lanes])
        sq = pre * pre
        t = jnp.tanh(TANH_SCALE * (pre + CUBIC * sq * pre))
        hidden[:, lanes] = (0.5 * pre * (1.0 + t)).astype(BF)
        deriv[:, lanes] = 0.5 * (1.0 + t) + 0.5 * pre * (1.0 - t * t) * TANH_SCALE * (
            1.0 + 3.0 * CUBIC * sq
        )
        return carry

    lax.fori_loop(0, hidden_units // step, feed, 0)
    loads[3].wait()
    u, iv = unit_of(DEPTH_GAIN * (unit1[...] * gain1) + nn(hidden[...], wback[...]))
    unit2[...] = u
    inv2[...] = iv

    grads = (
        (part_back, r1_back, r2_back, gback_ref),
        (part_in, r1_in, r2_in, gin_ref),
        (part_out, r1_out, r2_out, gout_ref),
        (part_qkv, r1_qkv, r2_qkv, gqkv_ref),
    )

    def near(g, i):
        part, r1, _, _ = grads[g]
        size = r1.shape[1]
        at = pl.multiple_of((2 * i + 1 - core) * size, size)
        return send(
            part.at[pl.ds(at, size)], r1.at[i], s1.at[g, i], q1.at[g, i],
            dp=2 * chip + 1 - core,
        )

    def far(g, o):
        _, r1, r2, _ = grads[g]
        i = lax.rem(chip + o, chips)
        return send(
            r1.at[i], r2.at[o - 1], s2.at[g, o - 1], q2.at[g, o - 1], dp=2 * i + core
        )

    def mine(g, i):
        part, r1, _, _ = grads[g]
        size = r1.shape[1]
        return part[pl.ds(pl.multiple_of((2 * i + core) * size, size), size)].astype(F32)

    def to_partner(g):
        for i in range(chips):
            near(g, i).start()

    def to_chips(g):
        r1 = grads[g][1]
        for i in range(chips):
            near(g, i).wait_recv()
        for o in range(1, chips):
            i = lax.rem(chip + o, chips)
            r1[i] = (r1[i].astype(F32) + mine(g, i)).astype(BF)
            far(g, o).start()

    def finish(g):
        _, r1, r2, out = grads[g]
        total = r1[chip].astype(F32) + mine(g, chip)
        for o in range(1, chips):
            far(g, o).wait_recv()
            total = total + r2[o - 1].astype(F32)
        out[...] = total.astype(out.dtype)

    def transposed(left, right, out):
        cols = min(step, left.shape[1])

        def body(i, carry):
            at = pl.ds(pl.multiple_of(i * cols, cols), cols)
            out[at, :] = tn(left[:, at], right).astype(BF)
            return carry

        lax.fori_loop(0, left.shape[1] // cols, body, 0)

    def backward(final):
        up = up_bf[...].astype(F32)
        d2, grad_two = norm_back(up, unit2[...], inv2[...], gain2)
        d2_bf = d2.astype(BF)
        dfirst[...] = DEPTH_GAIN * d2
        up_bf[...] = d2_bf

        if final:
            gsum[1:2, :] = grad_two
            transposed(hidden, up_bf[...], part_back)
            to_partner(0)

        def body(i, carry):
            lanes = pl.ds(pl.multiple_of(i * step, step), step)
            dh = nt(up_bf[...], wback[lanes, :])
            dpre[:, lanes] = (dh * deriv[:, lanes]).astype(BF)
            return carry

        lax.fori_loop(0, hidden_units // step, body, 0)
        if final:
            to_chips(0)
            transposed(normed_bf, dpre[...], part_in)
            to_partner(1)
        dn = dfirst[...] + nt(dpre[...], win[...])
        d1, grad_one = norm_back(dn, unit1[...], inv1[...], gain1)
        dfirst[...] = DEPTH_GAIN * d1
        up_bf[...] = d1.astype(BF)
        if final:
            gsum[0:1, :] = grad_one
            to_chips(1)
            transposed(ctx, up_bf[...], part_out)
            to_partner(2)
        dctx[...] = nt(up_bf[...], wout[...]).astype(BF)
        for s in range(sentences):
            rows = pl.ds(s * SEQ, SEQ)

            def attend(i, carry):
                lanes = lambda k: pl.ds(pl.multiple_of(k * width + i * 128, 128), 128)
                q, k, v = qkv[rows, lanes(0)], qkv[rows, lanes(1)], qkv[rows, lanes(2)]
                dc = dctx[rows, lanes(0)]
                outs = ([], [], [])
                for h in range(2):
                    cut = slice(h * HEAD_DIM, (h + 1) * HEAD_DIM)
                    p = probs[s, 2 * i + h]
                    dp_ = nt(dc[:, cut], v[:, cut])
                    outs[2].append(tn(p.astype(BF), dc[:, cut]))
                    ds = p * (dp_ - jnp.sum(p * dp_, axis=-1, keepdims=True)) * scale
                    ds = ds.astype(BF)
                    outs[0].append(nn(ds, k[:, cut]))
                    outs[1].append(tn(ds, q[:, cut]))
                for n in range(3):
                    dqkv[rows, lanes(n)] = jnp.concatenate(outs[n], axis=-1).astype(BF)
                return carry

            lax.fori_loop(0, pairs, attend, 0)
        if final:
            to_chips(2)
            transposed(x_ref, dqkv[...], part_qkv)
            to_partner(3)
        return (dfirst[...] + nt(dqkv[...], wqkv[...])).astype(BF)

    @pl.when(is_last)
    def _():
        up_bf[...] = cot_ref[...]

    @pl.when(layer < last)
    def _():
        up_guess().wait_recv()
        up_bf[...] = above[...]

    relaxed[...] = backward(False)
    plain_sender = (layer > 0) & jnp.logical_not(is_coarse)
    pl.when(plain_sender)(lambda: up_relaxed().start())
    coarse_sends(relaxed, crel, s_ce, r_ce, start, True)

    def build_err():
        here = jnp.int32(0)
        for i, t in tops:

            @pl.when(layer == t)
            def _():
                for idx in reversed(range(i, len(coarse))):
                    send(rate_ref, crate.at[idx], s_cr.at[0], r_cr.at[idx], layer=here).wait_recv()
                    if idx > i:
                        send(guess_ref, cguess.at[idx], s_cg.at[0], r_cg.at[idx], layer=here).wait_recv()
                    send(relaxed, crel.at[idx], s_ce.at[0], r_ce.at[idx], layer=here).wait_recv()
                    old = above[...] if idx == i else cguess[idx]
                    resid = crel[idx].astype(F32) - old.astype(F32)
                    above_it = idx < len(coarse) - 1
                    err[...] = crate[idx] * err[...] + resid if above_it else resid

        err_bf[...] = err[...].astype(BF)

    @pl.when(is_last)
    def _():
        up_bf[...] = cot_ref[...]

    @pl.when(next_plain)
    def _():
        up_relaxed().wait_recv()
        up_bf[...] = above2[...]

    @pl.when(next_coarse)
    def _():
        build_err()
        up_bf[...] = (above[...].astype(F32) + err[...]).astype(BF)
        lazy_sends(start)

    adj_ref[...] = backward(True)

    def gain_send(o):
        return send(
            gsum, grecv.at[o - 1], s_g.at[o - 1], r_g.at[o - 1], dp=lax.rem(dp + o, dpn)
        )

    for o in range(1, dpn):
        gain_send(o).start()
    to_chips(3)

    @pl.when(is_last)
    def _():
        err[...] = jnp.zeros_like(err)

    @pl.when(next_plain)
    def _():
        send(err_bf, err_in, s_lz.at[0], r_lz.at[0], layer=jnp.int32(0)).wait_recv()
        err[...] = err_in[...].astype(F32)

    @pl.when(is_coarse)
    def _():
        own = guess_ref[...].astype(F32)
        err[...] = rate_ref[...] * err[...] + (relaxed[...].astype(F32) - own)
        adj_ref[...] = (own + err[...]).astype(BF)

    err_ref[...] = err[...]
    finish(0)
    finish(1)
    gains = gsum[...]
    for o in range(1, dpn):
        gain_send(o).wait_recv()
        gains = gains + grecv[o - 1]
    piece = width // dpn
    one, two = jnp.zeros((1, piece), F32), jnp.zeros((1, piece), F32)
    for c in range(dpn):
        cut = slice(c * piece, (c + 1) * piece)
        here = dp == c
        one = one + jnp.where(here, gains[0:1, cut], 0.0)
        two = two + jnp.where(here, gains[1:2, cut], 0.0)
    g1_ref[...] = one
    g2_ref[...] = two
    finish(2)
    finish(3)

    sent = lambda c: c.wait_send()
    pl.when(layer > 0)(lambda: sent(up_guess()))
    pl.when(plain_sender)(lambda: sent(up_relaxed()))
    coarse_sends(guess_ref, cguess, s_cg, r_cg, sent, False)
    coarse_sends(rate_ref, crate, s_cr, r_cr, sent, True)
    coarse_sends(relaxed, crel, s_ce, r_ce, sent, True)
    lazy_sends(sent)
    for g in range(4):
        for i in range(chips):
            sent(near(g, i))
        for o in range(1, chips):
            sent(far(g, o))
    for o in range(1, dpn):
        sent(gain_send(o))


def writer(*refs):
    n = len(refs) // 2
    sems = refs[-1]
    copies = [
        pltpu.make_async_copy(refs[i], refs[n + i].at[0] if len(refs[n + i].shape) == 3 else refs[n + i], sems.at[i])
        for i in range(n)
    ]
    for copy in copies:
        copy.start()
    for copy in copies:
        copy.wait()


def on_device(layers, dpn, *args):
    (states, guess, cotangent, lengths, rate, w_qkv, w_out, w_in, w_back, gain1, gain2) = args
    tokens, width = states.shape[1:]
    ff = w_in.shape[2]
    heads = width // HEAD_DIM
    coarse = [j for j in range(1, layers) if j % FACTOR == 0 or j == layers - 1]
    n = len(coarse)
    chips = dpn // 2
    shapes = ((ff, width), (width, ff), (width, width), (width, 3 * width))
    vm = pltpu.VMEM
    rows = (tokens, width)
    dma = lambda *s: pltpu.SemaphoreType.DMA(s)
    line = vm((1, width), F32)
    scratch = [
        vm(rows, BF), vm(rows, BF), vm(rows, BF),
        line, line, line,
        vm((width, 3 * width), BF), vm((width, width), BF), vm((width, ff), BF),
        vm((ff, width), BF),
        vm((tokens, 3 * width), BF), vm((SEQ, SEQ), F32),
        vm((tokens // SEQ, heads, SEQ, SEQ), F32), vm(rows, BF), vm(rows, F32), vm(rows, F32),
        vm((tokens, 1), F32), vm((tokens, 1), F32), vm(rows, BF), vm((tokens, ff), BF),
        vm((tokens, ff), F32),
        vm(rows, BF), vm(rows, BF), vm((tokens, 3 * width), BF), vm((tokens, ff), BF),
        vm(rows, F32), vm(rows, BF),
        vm(rows, BF), vm(rows, BF), vm((n,) + rows, BF), vm((n,) + rows, BF),
        vm((n, 1, width), F32), vm(rows, F32), vm(rows, BF), vm(rows, BF),
    ]
    scratch += [vm(s, BF) for s in shapes]
    scratch += [vm((chips, s[0] // dpn, s[1]), BF) for s in shapes]
    scratch += [vm((max(chips - 1, 1), s[0] // dpn, s[1]), BF) for s in shapes]
    scratch += [vm((2, width), F32), vm((dpn - 1, 2, width), F32)]
    far = max(chips - 1, 1)
    scratch += [
        dma(4), dma(6), dma(2), dma(2), dma(n), dma(n), dma(n), dma(n), dma(n), dma(n),
        dma(FACTOR), dma(1),
        dma(4, chips), dma(4, chips), dma(4, far), dma(4, far), dma(dpn - 1), dma(dpn - 1),
    ]
    left = pl.BlockSpec(memory_space=pltpu.HBM)
    whole = pl.BlockSpec(memory_space=pltpu.VMEM)
    piece = lambda s: vm((s[0] // dpn, s[1]), F32)
    small = vm((1, width // dpn), F32)
    results = pl.pallas_call(
        functools.partial(kernel, layers, dpn, coarse),
        out_shape=(
            vm(rows, BF), vm(rows, F32), piece(shapes[3]), piece(shapes[2]), piece(shapes[1]),
            piece(shapes[0]), small, small,
        ),
        in_specs=[pl.BlockSpec(memory_space=pltpu.SMEM)] + [left] * 10,
        out_specs=(whole,) * 8,
        scratch_shapes=scratch,
        compiler_params=pltpu.CompilerParams(
            collective_id=0, has_side_effects=True, vmem_limit_bytes=48 * 1024 * 1024
        ),
    )(
        lengths,
        *(
            pltpu.with_memory_space_constraint(a, pltpu.HBM)
            for a in (
                states[0], guess[0], cotangent, rate, gain1, gain2,
                w_qkv[0], w_out[0], w_in[0], w_back[0],
            )
        )
    )
    results = [pltpu.with_memory_space_constraint(r, pltpu.VMEM) for r in results]
    shape = lambda r: r.shape if r.shape[0] == 1 else (1,) + r.shape
    return pl.pallas_call(
        writer,
        out_shape=tuple(jax.ShapeDtypeStruct(shape(r), r.dtype) for r in results),
        in_specs=[whole] * 8,
        out_specs=(left,) * 8,
        scratch_shapes=[dma(8)],
        compiler_params=pltpu.CompilerParams(vmem_limit_bytes=1024 * 1024),
    )(*results)


def solution(mesh):
    placed = (
        P("layer", "dp", None), P("layer", "dp", None), P("dp", None), P("dp"),
        P("layer", None), P("layer", None, None), P("layer", None, None),
        P("layer", None, None), P("layer", None, None), P("layer", None), P("layer", None),
    )
    split = P("layer", "dp", None)
    return jax.shard_map(
        functools.partial(on_device, mesh.shape["layer"], mesh.shape["dp"]),
        mesh=mesh,
        in_specs=placed,
        out_specs=(split,) * 6 + (P("layer", "dp"),) * 2,
        check_vma=False,
    )
```

```python
import functools

import jax
import jax.numpy as jnp
from jax import lax
from jax.experimental import pallas as pl
from jax.experimental.pallas import tpu as pltpu
from jax.sharding import PartitionSpec as P

HEAD_DIM = 64
SEQ = 256
FACTOR = 4
EPS = 1e-05
DEPTH_GAIN = 6.73
CUBIC = 0.044715
TANH_SCALE = 0.7978845608028654
F32 = jnp.float32
BF = jnp.bfloat16


def nn(a, b):
    return lax.dot_general(a, b, (((1,), (0,)), ((), ())), preferred_element_type=F32)


def nt(a, b):
    return lax.dot_general(a, b, (((1,), (1,)), ((), ())), preferred_element_type=F32)


def tn(a, b):
    return lax.dot_general(a, b, (((0,), (0,)), ((), ())), preferred_element_type=F32)


def mean(v):
    return jnp.mean(v, axis=-1, keepdims=True)


def unit_of(v):
    center = v - mean(v)
    inv = lax.rsqrt(mean(center * center) + EPS)
    return center * inv, inv


def norm_back(up, unit, inv, gain):
    scaled = up * gain
    inner = scaled - mean(scaled) - unit * mean(scaled * unit)
    return inv * inner, jnp.sum(up * unit, axis=0, keepdims=True)


def kernel(
    layers, dpn, coarse,
    len_ref, x_hbm, guess_hbm, cot_hbm, rate_hbm, gain1_hbm, gain2_hbm,
    wqkv_hbm, wout_hbm, win_hbm, wback_hbm,
    adj_ref, err_ref, gqkv_ref, gout_ref, gin_ref, gback_ref, g1_ref, g2_ref,
    x_ref, guess_ref, cot_ref, rate_ref, gain1_ref, gain2_ref,
    wqkv, wout, win, wback,
    qkv, bias, probs, ctx, unit1, unit2, inv1, inv2, normed_bf, hidden, deriv,
    up_bf, dctx, dqkv, dpre, dfirst, relaxed,
    above, above2, crel, cguess, crate, err, err_bf, err_in,
    part_back, part_in, part_out, part_qkv,
    r1_back, r1_in, r1_out, r1_qkv,
    r2_back, r2_in, r2_out, r2_qkv,
    gsum, grecv,
    x_far, ctx_far, normed_far, d2_far, d1_far, dpre_far, d2_bf, unit1_far, inv1_far,
    hidden_far, deriv_far, x_t, half_s, half_r, quarter_s, quarter_r, small_s, small_r,
    pq, pq1, pq2,
    wsem, lsem, s_up, r_up, s_cg, r_cg, s_cr, r_cr, s_ce, r_ce, s_lz, r_lz,
    s1, q1, s2, q2, s_g, r_g, s_mate, r_mate, s_half, r_half, sq1, rq1, sq2, rq2,
):
    layer = lax.axis_index("layer")
    dp = lax.axis_index("dp")
    tokens, width = x_ref.shape
    hidden_units = hidden.shape[1]
    sentences = tokens // SEQ
    pairs = width // 128
    scale = HEAD_DIM ** (-0.5)
    chips = dpn // 2
    chip, core = dp // 2, dp % 2
    paired = chips == 2
    mate, sibling = 2 * (1 - chip) + core, 2 * chip + 1 - core
    last = layers - 1
    is_last = layer == last
    is_coarse = (layer % FACTOR == 0) | is_last
    next_coarse = (((layer + 1) % FACTOR == 0) | (layer + 1 == last)) & (layer < last)
    next_plain = (layer < last) & (((layer + 1) % FACTOR != 0) & (layer + 1 != last))

    def send(src, dst, ssem, rsem, **where):
        return pltpu.make_async_remote_copy(
            src_ref=src, dst_ref=dst, send_sem=ssem, recv_sem=rsem,
            device_id=where, device_id_type=pl.DeviceIdType.MESH,
        )

    loads = [
        pltpu.make_async_copy(a, b, wsem.at[i])
        for i, (a, b) in enumerate(
            ((wqkv_hbm, wqkv), (wout_hbm, wout), (win_hbm, win), (wback_hbm, wback))
        )
    ]
    small = [
        pltpu.make_async_copy(a, b, lsem.at[i])
        for i, (a, b) in enumerate(
            (
                (x_hbm, x_ref), (guess_hbm, guess_ref), (rate_hbm, rate_ref),
                (gain1_hbm, gain1_ref), (gain2_hbm, gain2_ref),
                (cot_hbm, cot_ref),
            )
        )
    ]
    for load in small[:3] + loads[:1] + small[3:] + loads[1:]:
        load.start()

    barrier = pltpu.get_barrier_semaphore()
    for o in range(1, layers):
        pl.semaphore_signal(
            barrier, inc=1, device_id={"layer": lax.rem(layer + o, layers)},
            device_id_type=pl.DeviceIdType.MESH,
        )
    for o in range(1, dpn):
        pl.semaphore_signal(
            barrier, inc=1, device_id={"dp": lax.rem(dp + o, dpn)},
            device_id_type=pl.DeviceIdType.MESH,
        )
    pl.semaphore_wait(barrier, layers - 1 + dpn - 1)

    tops = [(i, c - 1) for i, c in enumerate(coarse)]

    up_guess = lambda: send(
        guess_ref, above, s_up.at[0], r_up.at[0], layer=jnp.maximum(layer - 1, 0)
    )
    up_relaxed = lambda: send(
        relaxed, above2, s_up.at[1], r_up.at[1], layer=jnp.maximum(layer - 1, 0)
    )

    def coarse_sends(src, dst, ssem, rsem, act, own):
        for idx, j in enumerate(coarse):
            reach = [t for i, t in tops if i < idx or (own and i == idx)]
            if reach:

                @pl.when(layer == j)
                def _():
                    for n, t in enumerate(reach[::-1]):
                        act(send(src, dst.at[idx], ssem.at[n], rsem.at[idx], layer=jnp.int32(t)))

    def lazy_sends(act):
        for i, t in tops:
            low = coarse[i - 1] if i else 0

            @pl.when(layer == t)
            def _():
                for n, target in enumerate(range(low, t)):
                    act(send(err_bf, err_in, s_lz.at[n], r_lz.at[0], layer=jnp.int32(target)))

    for load in small[1:3]:
        load.wait()
    pl.when(layer > 0)(lambda: up_guess().start())
    start = lambda c: c.start()
    coarse_sends(rate_ref, crate, s_cr, r_cr, start, True)
    coarse_sends(guess_ref, cguess, s_cg, r_cg, start, False)
    small[0].wait()
    to_mate = lambda i, src, dst: send(src, dst, s_mate.at[i], r_mate.at[i], dp=mate)
    mate_x = lambda: to_mate(0, x_ref, x_far)
    mate_ctx = lambda: to_mate(1, ctx, ctx_far)
    mate_d2 = lambda: to_mate(2, d2_bf, d2_far)
    if paired:
        mate_x().start()
    for load in small[3:]:
        load.wait()

    gain1, gain2 = gain1_ref[...], gain2_ref[...]
    loads[0].wait()
    qkv[...] = nn(x_ref[...], wqkv[...]).astype(BF)
    for s in range(sentences):
        rows = pl.ds(s * SEQ, SEQ)
        row_at = lax.broadcasted_iota(jnp.int32, (SEQ, SEQ), 0)
        col_at = lax.broadcasted_iota(jnp.int32, (SEQ, SEQ), 1)
        bias[...] = jnp.where((col_at <= row_at) & (col_at < len_ref[s]), 0.0, -1e30)

        def attend(i, carry):
            lanes = lambda k: pl.ds(pl.multiple_of(k * width + i * 128, 128), 128)
            q, k, v = qkv[rows, lanes(0)], qkv[rows, lanes(1)], qkv[rows, lanes(2)]
            outs = []
            for h in range(2):
                cut = slice(h * HEAD_DIM, (h + 1) * HEAD_DIM)
                sc = nt(q[:, cut], k[:, cut]) * scale + bias[...]
                e = jnp.exp(sc - jnp.max(sc, axis=-1, keepdims=True))
                p = e * (1.0 / jnp.sum(e, axis=-1, keepdims=True))
                probs[s, 2 * i + h] = p
                outs.append(nn(p.astype(BF), v[:, cut]))
            ctx[rows, lanes(0)] = jnp.concatenate(outs, axis=-1).astype(BF)
            return carry

        lax.fori_loop(0, pairs, attend, 0)
    if paired:
        mate_ctx().start()
    loads[1].wait()
    u, iv = unit_of(DEPTH_GAIN * x_ref[...].astype(F32) + nn(ctx[...], wout[...]))
    unit1[...] = u
    inv1[...] = iv
    normed_bf[...] = (u * gain1).astype(BF)
    loads[2].wait()
    step = 512

    def feed_forward(normed, out, slope):
        def feed(i, carry):
            lanes = pl.ds(pl.multiple_of(i * step, step), step)
            pre = nn(normed[...], win[:, lanes])
            sq = pre * pre
            t = jnp.tanh(TANH_SCALE * (pre + CUBIC * sq * pre))
            out[:, lanes] = (0.5 * pre * (1.0 + t)).astype(BF)
            slope[:, lanes] = 0.5 * (1.0 + t) + 0.5 * pre * (1.0 - t * t) * TANH_SCALE * (
                1.0 + 3.0 * CUBIC * sq
            )
            return carry

        with jax.named_scope("feed"):
            lax.fori_loop(0, hidden_units // step, feed, 0)

    feed_forward(normed_bf, hidden, deriv)
    loads[3].wait()
    u, iv = unit_of(DEPTH_GAIN * (unit1[...] * gain1) + nn(hidden[...], wback[...]))
    unit2[...] = u
    inv2[...] = iv

    grads = (
        (part_back, r1_back, r2_back, gback_ref),
        (part_in, r1_in, r2_in, gin_ref),
        (part_out, r1_out, r2_out, gout_ref),
        (part_qkv, r1_qkv, r2_qkv, gqkv_ref),
    )

    def near(g, i):
        part, r1, _, _ = grads[g]
        size = r1.shape[1]
        at = pl.multiple_of((2 * i + 1 - core) * size, size)
        return send(
            part.at[pl.ds(at, size)], r1.at[i], s1.at[g, i], q1.at[g, i],
            dp=2 * chip + 1 - core,
        )

    def far(g, o):
        _, r1, r2, _ = grads[g]
        i = lax.rem(chip + o, chips)
        return send(
            r1.at[i], r2.at[o - 1], s2.at[g, o - 1], q2.at[g, o - 1], dp=2 * i + core
        )

    def mine(g, i):
        part, r1, _, _ = grads[g]
        size = r1.shape[1]
        return part[pl.ds(pl.multiple_of((2 * i + core) * size, size), size)].astype(F32)

    def to_partner(g):
        for i in range(chips):
            near(g, i).start()

    def to_chips(g):
        r1 = grads[g][1]
        for i in range(chips):
            near(g, i).wait_recv()
        for o in range(1, chips):
            i = lax.rem(chip + o, chips)
            r1[i] = (r1[i].astype(F32) + mine(g, i)).astype(BF)
            far(g, o).start()

    def finish(g):
        _, r1, r2, out = grads[g]
        total = r1[chip].astype(F32) + mine(g, chip)
        for o in range(1, chips):
            far(g, o).wait_recv()
            total = total + r2[o - 1].astype(F32)
        out[...] = total.astype(out.dtype)

    def transposed(left, right, out):
        cols = min(step, left.shape[1])

        def body(i, carry):
            at = pl.ds(pl.multiple_of(i * cols, cols), cols)
            out[at, :] = tn(left[:, at], right).astype(BF)
            return carry

        lax.fori_loop(0, left.shape[1] // cols, body, 0)

    def hidden_back(d, slope, out):
        def body(i, carry):
            lanes = pl.ds(pl.multiple_of(i * step, step), step)
            out[:, lanes] = (nt(d[...], wback[lanes, :]) * slope[:, lanes]).astype(BF)
            return carry

        with jax.named_scope("du"):
            lax.fori_loop(0, hidden_units // step, body, 0)

    def attend_back(s, i):
        rows = pl.ds(s * SEQ, SEQ)
        lanes = lambda k: pl.ds(pl.multiple_of(k * width + i * 128, 128), 128)
        q, k, v = qkv[rows, lanes(0)], qkv[rows, lanes(1)], qkv[rows, lanes(2)]
        dc = dctx[rows, lanes(0)]
        outs = ([], [], [])
        for h in range(2):
            cut = slice(h * HEAD_DIM, (h + 1) * HEAD_DIM)
            p = probs[s, 2 * i + h]
            dp_ = nt(dc[:, cut], v[:, cut])
            outs[2].append(tn(p.astype(BF), dc[:, cut]))
            ds = p * (dp_ - jnp.sum(p * dp_, axis=-1, keepdims=True)) * scale
            ds = ds.astype(BF)
            outs[0].append(nn(ds, k[:, cut]))
            outs[1].append(tn(ds, q[:, cut]))
        for n in range(3):
            dqkv[rows, lanes(n)] = jnp.concatenate(outs[n], axis=-1).astype(BF)

    def backward(final):
        up = up_bf[...].astype(F32)
        d2, grad_two = norm_back(up, unit2[...], inv2[...], gain2)
        d2_bf = d2.astype(BF)
        dfirst[...] = DEPTH_GAIN * d2
        up_bf[...] = d2_bf

        if final:
            gsum[1:2, :] = grad_two
            transposed(hidden, up_bf[...], part_back)
            to_partner(0)

        hidden_back(up_bf, deriv, dpre)
        if final:
            to_chips(0)
            transposed(normed_bf, dpre[...], part_in)
            to_partner(1)
        dn = dfirst[...] + nt(dpre[...], win[...])
        d1, grad_one = norm_back(dn, unit1[...], inv1[...], gain1)
        dfirst[...] = DEPTH_GAIN * d1
        up_bf[...] = d1.astype(BF)
        if final:
            gsum[0:1, :] = grad_one
            to_chips(1)
            transposed(ctx, up_bf[...], part_out)
            to_partner(2)
        dctx[...] = nt(up_bf[...], wout[...]).astype(BF)
        for s in range(sentences):

            def attend(i, carry):
                attend_back(s, i)
                return carry

            with jax.named_scope("att2"):
                lax.fori_loop(0, pairs, attend, 0)
        if final:
            to_chips(2)
            transposed(x_ref, dqkv[...], part_qkv)
            to_partner(3)
        return (dfirst[...] + nt(dqkv[...], wqkv[...])).astype(BF)

    def half_send(g):
        src, dst = ((half_s, half_r), (quarter_s, quarter_r), (small_s, small_r))[g]
        return send(src, dst, s_half.at[g], r_half.at[g], dp=sibling)

    def near_qkv(i, c):
        size = pq.shape[1] // dpn
        at = pl.multiple_of((2 * c + 1 - core) * size, size)
        return send(
            pq.at[i, pl.ds(at, size)], pq1.at[i, c], sq1.at[i, c], rq1.at[i, c], dp=sibling
        )

    def mine_qkv(i, c):
        size = pq.shape[1] // dpn
        at = pl.multiple_of((2 * c + core) * size, size)
        return pq[i, pl.ds(at, size)].astype(F32)

    def far_qkv(i):
        return send(pq1.at[i, 1 - chip], pq2.at[i], sq2.at[i], rq2.at[i], dp=mate)

    def relay_qkv(i):
        near_qkv(i, 1 - chip).wait_recv()
        pq1[i, 1 - chip] = (pq1[i, 1 - chip].astype(F32) + mine_qkv(i, 1 - chip)).astype(BF)
        far_qkv(i).start()

    def finish_qkv(i):
        near_qkv(i, chip).wait_recv()
        total = pq1[i, chip].astype(F32) + mine_qkv(i, chip)
        far_qkv(i).wait_recv()
        total = total + pq2[i].astype(F32)
        for n in range(3):
            gqkv_ref[:, n * width + i * 128 : n * width + (i + 1) * 128] = total[
                :, n * 128 : (n + 1) * 128
            ]

    def rows_of(left, left_far, right, right_far, c, size):
        at = pl.ds(pl.multiple_of((2 * chip + c) * size, size), size)
        return tn(left[:, at], right[...]) + tn(left_far[:, at], right_far[...])

    def look_ahead():
        mate_x().wait_recv()
        mate_ctx().wait_recv()
        u, iv = unit_of(DEPTH_GAIN * x_far[...].astype(F32) + nn(ctx_far[...], wout[...]))
        unit1_far[...] = u
        inv1_far[...] = iv
        normed_far[...] = (u * gain1).astype(BF)
        feed_forward(normed_far, hidden_far, deriv_far)
        x_t[...] = x_ref[...].T

    def backward_paired():
        d2, grad_two = norm_back(up_bf[...].astype(F32), unit2[...], inv2[...], gain2)
        d2_bf[...] = d2.astype(BF)
        mate_d2().start()
        dfirst[...] = DEPTH_GAIN * d2
        gsum[1:2, :] = grad_two
        hidden_back(d2_bf, deriv, dpre)
        d1, grad_one = norm_back(dfirst[...] + nt(dpre[...], win[...]), unit1[...], inv1[...], gain1)
        dfirst[...] = DEPTH_GAIN * d1
        up_bf[...] = d1.astype(BF)
        gsum[0:1, :] = grad_one
        for o in range(1, dpn):
            gain_send(o).start()
        dctx[...] = nt(up_bf[...], wout[...]).astype(BF)
        for i in range(pairs):
            with jax.named_scope("att2"):
                for s in range(sentences):
                    attend_back(s, i)
            with jax.named_scope("gqkv"):
                cut = [dqkv[:, n * width + i * 128 : n * width + (i + 1) * 128] for n in range(3)]
                pq[i] = nn(x_t[...], jnp.concatenate(cut, axis=-1)).astype(BF)
                near_qkv(i, 1 - chip).start()
                near_qkv(i, chip).start()
            if i:
                relay_qkv(i - 1)
        with jax.named_scope("wd2"):
            mate_d2().wait_recv()
        hidden_back(d2_far, deriv_far, dpre_far)
        relay_qkv(pairs - 1)
        d2o = d2_far[...].astype(F32)
        d1, _ = norm_back(
            DEPTH_GAIN * d2o + nt(dpre_far[...], win[...]), unit1_far[...], inv1_far[...], gain1
        )
        d1_far[...] = d1.astype(BF)
        parts = (
            (hidden, hidden_far, d2_bf, d2_far, half_s, gback_ref),
            (normed_bf, normed_far, dpre, dpre_far, quarter_s, gin_ref),
            (ctx, ctx_far, up_bf, d1_far, small_s, gout_ref),
        )
        with jax.named_scope("gpart"):
            for g, (a, a_far, b, b_far, out, _) in enumerate(parts):
                out[...] = rows_of(a, a_far, b, b_far, 1 - core, out.shape[0]).astype(BF)
                half_send(g).start()
            for a, a_far, b, b_far, _, out in parts:
                out[...] = rows_of(a, a_far, b, b_far, core, out.shape[0])
        return (dfirst[...] + nt(dqkv[...], wqkv[...])).astype(BF)

    def gain_send(o):
        return send(
            gsum, grecv.at[o - 1], s_g.at[o - 1], r_g.at[o - 1], dp=lax.rem(dp + o, dpn)
        )

    @pl.when(is_last)
    def _():
        up_bf[...] = cot_ref[...]

    @pl.when(layer < last)
    def _():
        up_guess().wait_recv()
        up_bf[...] = above[...]

    relaxed[...] = backward(False)
    plain_sender = (layer > 0) & jnp.logical_not(is_coarse)
    pl.when(plain_sender)(lambda: up_relaxed().start())
    coarse_sends(relaxed, crel, s_ce, r_ce, start, True)
    if paired:
        look_ahead()

    def build_err():
        here = jnp.int32(0)
        for i, t in tops:

            @pl.when(layer == t)
            def _():
                for idx in reversed(range(i, len(coarse))):
                    send(rate_ref, crate.at[idx], s_cr.at[0], r_cr.at[idx], layer=here).wait_recv()
                    if idx > i:
                        send(guess_ref, cguess.at[idx], s_cg.at[0], r_cg.at[idx], layer=here).wait_recv()
                    send(relaxed, crel.at[idx], s_ce.at[0], r_ce.at[idx], layer=here).wait_recv()
                    old = above[...] if idx == i else cguess[idx]
                    resid = crel[idx].astype(F32) - old.astype(F32)
                    above_it = idx < len(coarse) - 1
                    err[...] = crate[idx] * err[...] + resid if above_it else resid

        err_bf[...] = err[...].astype(BF)

    @pl.when(is_last)
    def _():
        up_bf[...] = cot_ref[...]

    @pl.when(next_plain)
    def _():
        up_relaxed().wait_recv()
        up_bf[...] = above2[...]

    @pl.when(next_coarse)
    def _():
        build_err()
        up_bf[...] = (above[...].astype(F32) + err[...]).astype(BF)
        lazy_sends(start)

    if paired:
        adj_ref[...] = backward_paired()
    else:
        adj_ref[...] = backward(True)
        for o in range(1, dpn):
            gain_send(o).start()
        to_chips(3)

    @pl.when(is_last)
    def _():
        err[...] = jnp.zeros_like(err)

    @pl.when(next_plain)
    def _():
        send(err_bf, err_in, s_lz.at[0], r_lz.at[0], layer=jnp.int32(0)).wait_recv()
        err[...] = err_in[...].astype(F32)

    @pl.when(is_coarse)
    def _():
        own = guess_ref[...].astype(F32)
        err[...] = rate_ref[...] * err[...] + (relaxed[...].astype(F32) - own)
        adj_ref[...] = (own + err[...]).astype(BF)

    err_ref[...] = err[...]
    if not paired:
        finish(0)
        finish(1)
    gains = gsum[...]
    for o in range(1, dpn):
        gain_send(o).wait_recv()
        gains = gains + grecv[o - 1]
    piece = width // dpn
    one, two = jnp.zeros((1, piece), F32), jnp.zeros((1, piece), F32)
    for c in range(dpn):
        cut = slice(c * piece, (c + 1) * piece)
        here = dp == c
        one = one + jnp.where(here, gains[0:1, cut], 0.0)
        two = two + jnp.where(here, gains[1:2, cut], 0.0)
    g1_ref[...] = one
    g2_ref[...] = two
    if paired:
        for g, (part, out) in enumerate(
            ((half_r, gback_ref), (quarter_r, gin_ref), (small_r, gout_ref))
        ):
            half_send(g).wait_recv()
            out[...] = out[...] + part[...].astype(F32)
        with jax.named_scope("finq"):
            for i in range(pairs):
                finish_qkv(i)
    else:
        finish(2)
        finish(3)

    sent = lambda c: c.wait_send()
    pl.when(layer > 0)(lambda: sent(up_guess()))
    pl.when(plain_sender)(lambda: sent(up_relaxed()))
    coarse_sends(guess_ref, cguess, s_cg, r_cg, sent, False)
    coarse_sends(rate_ref, crate, s_cr, r_cr, sent, True)
    coarse_sends(relaxed, crel, s_ce, r_ce, sent, True)
    lazy_sends(sent)
    if paired:
        for copy in (mate_x(), mate_ctx(), mate_d2()):
            sent(copy)
        for g in range(3):
            sent(half_send(g))
        for i in range(pairs):
            sent(near_qkv(i, 0))
            sent(near_qkv(i, 1))
            sent(far_qkv(i))
    else:
        for g in range(4):
            for i in range(chips):
                sent(near(g, i))
            for o in range(1, chips):
                sent(far(g, o))
    for o in range(1, dpn):
        sent(gain_send(o))


def writer(*refs):
    n = len(refs) // 2
    sems = refs[-1]
    copies = [
        pltpu.make_async_copy(refs[i], refs[n + i].at[0] if len(refs[n + i].shape) == 3 else refs[n + i], sems.at[i])
        for i in range(n)
    ]
    for copy in copies:
        copy.start()
    for copy in copies:
        copy.wait()


def on_device(layers, dpn, *args):
    (states, guess, cotangent, lengths, rate, w_qkv, w_out, w_in, w_back, gain1, gain2) = args
    tokens, width = states.shape[1:]
    ff = w_in.shape[2]
    heads = width // HEAD_DIM
    coarse = [j for j in range(1, layers) if j % FACTOR == 0 or j == layers - 1]
    n = len(coarse)
    chips = dpn // 2
    shapes = ((ff, width), (width, ff), (width, width), (width, 3 * width))
    vm = pltpu.VMEM
    rows = (tokens, width)
    dma = lambda *s: pltpu.SemaphoreType.DMA(s)
    line = vm((1, width), F32)
    scratch = [
        vm(rows, BF), vm(rows, BF), vm(rows, BF),
        line, line, line,
        vm((width, 3 * width), BF), vm((width, width), BF), vm((width, ff), BF),
        vm((ff, width), BF),
        vm((tokens, 3 * width), BF), vm((SEQ, SEQ), F32),
        vm((tokens // SEQ, heads, SEQ, SEQ), F32), vm(rows, BF), vm(rows, F32), vm(rows, F32),
        vm((tokens, 1), F32), vm((tokens, 1), F32), vm(rows, BF), vm((tokens, ff), BF),
        vm((tokens, ff), F32),
        vm(rows, BF), vm(rows, BF), vm((tokens, 3 * width), BF), vm((tokens, ff), BF),
        vm(rows, F32), vm(rows, BF),
        vm(rows, BF), vm(rows, BF), vm((n,) + rows, BF), vm((n,) + rows, BF),
        vm((n, 1, width), F32), vm(rows, F32), vm(rows, BF), vm(rows, BF),
    ]
    paired = chips == 2
    pairs = width // 128
    far = max(chips - 1, 1)
    tile = (8, 128)
    either = lambda use, s, t=BF: vm(s if use else tile, t)
    scratch += [either(not paired, s) for s in shapes]
    scratch += [either(not paired, (chips, s[0] // dpn, s[1])) for s in shapes]
    scratch += [either(not paired, (far, s[0] // dpn, s[1])) for s in shapes]
    scratch += [vm((2, width), F32), vm((dpn - 1, 2, width), F32)]
    scratch += [either(paired, rows) for _ in range(5)]
    scratch += [
        either(paired, (tokens, ff)), either(paired, rows), either(paired, rows, F32),
        either(paired, (tokens, 1), F32), either(paired, (tokens, ff)),
        either(paired, (tokens, ff), F32), either(paired, (width, tokens)),
    ]
    for s in (shapes[0], shapes[1], shapes[2]):
        scratch += [either(paired, (s[0] // dpn, s[1])) for _ in range(2)]
    scratch += [
        either(paired, (pairs, width, 384)), either(paired, (pairs, 2, width // dpn, 384)),
        either(paired, (pairs, width // dpn, 384)),
    ]
    scratch += [
        dma(4), dma(6), dma(2), dma(2), dma(n), dma(n), dma(n), dma(n), dma(n), dma(n),
        dma(FACTOR), dma(1),
        dma(4, chips), dma(4, chips), dma(4, far), dma(4, far), dma(dpn - 1), dma(dpn - 1),
        dma(3), dma(3), dma(3), dma(3), dma(pairs, 2), dma(pairs, 2), dma(pairs), dma(pairs),
    ]
    left = pl.BlockSpec(memory_space=pltpu.HBM)
    whole = pl.BlockSpec(memory_space=pltpu.VMEM)
    piece = lambda s: vm((s[0] // dpn, s[1]), F32)
    small = vm((1, width // dpn), F32)
    results = pl.pallas_call(
        functools.partial(kernel, layers, dpn, coarse),
        out_shape=(
            vm(rows, BF), vm(rows, F32), piece(shapes[3]), piece(shapes[2]), piece(shapes[1]),
            piece(shapes[0]), small, small,
        ),
        in_specs=[pl.BlockSpec(memory_space=pltpu.SMEM)] + [left] * 10,
        out_specs=(whole,) * 8,
        scratch_shapes=scratch,
        compiler_params=pltpu.CompilerParams(
            collective_id=0, has_side_effects=True, vmem_limit_bytes=48 * 1024 * 1024
        ),
    )(
        lengths,
        *(
            pltpu.with_memory_space_constraint(a, pltpu.HBM)
            for a in (
                states[0], guess[0], cotangent, rate, gain1, gain2,
                w_qkv[0], w_out[0], w_in[0], w_back[0],
            )
        )
    )
    results = [pltpu.with_memory_space_constraint(r, pltpu.VMEM) for r in results]
    shape = lambda r: r.shape if r.shape[0] == 1 else (1,) + r.shape
    return pl.pallas_call(
        writer,
        out_shape=tuple(jax.ShapeDtypeStruct(shape(r), r.dtype) for r in results),
        in_specs=[whole] * 8,
        out_specs=(left,) * 8,
        scratch_shapes=[dma(8)],
        compiler_params=pltpu.CompilerParams(vmem_limit_bytes=1024 * 1024),
    )(*results)


def solution(mesh):
    placed = (
        P("layer", "dp", None), P("layer", "dp", None), P("dp", None), P("dp"),
        P("layer", None), P("layer", None, None), P("layer", None, None),
        P("layer", None, None), P("layer", None, None), P("layer", None), P("layer", None),
    )
    split = P("layer", "dp", None)
    return jax.shard_map(
        functools.partial(on_device, mesh.shape["layer"], mesh.shape["dp"]),
        mesh=mesh,
        in_specs=placed,
        out_specs=(split,) * 6 + (P("layer", "dp"),) * 2,
        check_vma=False,
    )
```

```python
import functools

import jax
import jax.numpy as jnp
from jax import lax
from jax.experimental import pallas as pl
from jax.experimental.pallas import tpu as pltpu
from jax.sharding import PartitionSpec as P

HEAD_DIM = 64
SEQ = 256
FACTOR = 4
EPS = 1e-05
DEPTH_GAIN = 6.73
CUBIC = 0.044715
TANH_SCALE = 0.7978845608028654
F32 = jnp.float32
BF = jnp.bfloat16


def nn(a, b):
    return lax.dot_general(a, b, (((1,), (0,)), ((), ())), preferred_element_type=F32)


def nt(a, b):
    return lax.dot_general(a, b, (((1,), (1,)), ((), ())), preferred_element_type=F32)


def tn(a, b):
    return lax.dot_general(a, b, (((0,), (0,)), ((), ())), preferred_element_type=F32)


def mean(v):
    return jnp.mean(v, axis=-1, keepdims=True)


def unit_of(v):
    center = v - mean(v)
    inv = lax.rsqrt(mean(center * center) + EPS)
    return center * inv, inv


def norm_back(up, unit, inv, gain):
    scaled = up * gain
    inner = scaled - mean(scaled) - unit * mean(scaled * unit)
    return inv * inner, jnp.sum(up * unit, axis=0, keepdims=True)


def kernel(
    layers, dpn, coarse, cuts,
    len_ref, x_hbm, guess_hbm, cot_hbm, rate_hbm, gain1_hbm, gain2_hbm,
    wqkv_hbm, wout_hbm, win_hbm, wback_hbm,
    adj_ref, err_ref, gqkv_ref, gout_ref, gin_ref, gback_ref, g1_ref, g2_ref,
    x_ref, guess_ref, cot_ref, rate_ref, gain1_ref, gain2_ref,
    wqkv, wout, win, wback,
    qkv, bias, probs, ctx, unit1, unit2, inv1, inv2, normed_bf, hidden, deriv,
    up_bf, dctx, dqkv, dpre, dfirst, relaxed,
    above, above2, crel, cguess, crate, err, err_bf, err_in,
    part_back, part_in, part_out, part_qkv,
    r1_back, r1_in, r1_out, r1_qkv,
    r2_back, r2_in, r2_out, r2_qkv,
    gsum, grecv,
    x_far, ctx_far, normed_far, d2_far, d1_far, dpre_far, d2_bf, unit1_far, inv1_far,
    hidden_far, deriv_far, x_t, half_s, half_r, quarter_s, quarter_r, small_s, small_r,
    pq, pq1, pq2, q_t, dctx_t,
    wsem, lsem, s_up, r_up, s_cg, r_cg, s_cr, r_cr, s_ce, r_ce, s_lz, r_lz,
    s1, q1, s2, q2, s_g, r_g, s_mate, r_mate, s_half, r_half, sq1, rq1, sq2, rq2,
):
    layer = lax.axis_index("layer")
    dp = lax.axis_index("dp")
    tokens, width = x_ref.shape
    hidden_units = hidden.shape[1]
    sentences = tokens // SEQ
    pairs = width // 128
    scale = HEAD_DIM ** (-0.5)
    chips = dpn // 2
    chip, core = dp // 2, dp % 2
    paired = chips == 2
    mate, sibling = 2 * (1 - chip) + core, 2 * chip + 1 - core
    last = layers - 1
    is_last = layer == last
    is_coarse = (layer % FACTOR == 0) | is_last
    next_coarse = (((layer + 1) % FACTOR == 0) | (layer + 1 == last)) & (layer < last)
    next_plain = (layer < last) & (((layer + 1) % FACTOR != 0) & (layer + 1 != last))

    def send(src, dst, ssem, rsem, **where):
        return pltpu.make_async_remote_copy(
            src_ref=src, dst_ref=dst, send_sem=ssem, recv_sem=rsem,
            device_id=where, device_id_type=pl.DeviceIdType.MESH,
        )

    loads = [
        pltpu.make_async_copy(a, b, wsem.at[i])
        for i, (a, b) in enumerate(
            ((wqkv_hbm, wqkv), (wout_hbm, wout), (win_hbm, win), (wback_hbm, wback))
        )
    ]
    small = [
        pltpu.make_async_copy(a, b, lsem.at[i])
        for i, (a, b) in enumerate(
            (
                (x_hbm, x_ref), (guess_hbm, guess_ref), (rate_hbm, rate_ref),
                (gain1_hbm, gain1_ref), (gain2_hbm, gain2_ref),
                (cot_hbm, cot_ref),
            )
        )
    ]
    for load in small[:1] + loads[:1] + small[1:] + loads[1:]:
        load.start()

    barrier = pltpu.get_barrier_semaphore()
    for o in range(1, layers):
        pl.semaphore_signal(
            barrier, inc=1, device_id={"layer": lax.rem(layer + o, layers)},
            device_id_type=pl.DeviceIdType.MESH,
        )
    for o in range(1, dpn):
        pl.semaphore_signal(
            barrier, inc=1, device_id={"dp": lax.rem(dp + o, dpn)},
            device_id_type=pl.DeviceIdType.MESH,
        )
    tops = [(i, c - 1) for i, c in enumerate(coarse)]

    part_rows = tokens // cuts
    span = lambda r: pl.ds(r * part_rows, part_rows)
    down = jnp.maximum(layer - 1, 0)

    def up_guess(r):
        at = span(r)
        return send(guess_ref.at[at], above.at[at], s_up.at[0, r], r_up.at[0, r], layer=down)

    def up_relaxed(r):
        at = span(r)
        return send(relaxed.at[at], above2.at[at], s_up.at[1, r], r_up.at[1, r], layer=down)

    def crel_send(idx, n, r, target):
        at = span(r)
        return send(
            relaxed.at[at], crel.at[idx, at], s_ce.at[n, r], r_ce.at[idx, r], layer=target
        )

    def crel_sends(r, act):
        for idx, j in enumerate(coarse):

            @pl.when(layer == j)
            def _():
                for n in range(idx + 1):
                    act(crel_send(idx, n, r, jnp.int32(coarse[idx - n] - 1)))

    def coarse_sends(src, dst, ssem, rsem, act, own):
        for idx, j in enumerate(coarse):
            reach = [t for i, t in tops if i < idx or (own and i == idx)]
            if reach:

                @pl.when(layer == j)
                def _():
                    for n, t in enumerate(reach[::-1]):
                        act(send(src, dst.at[idx], ssem.at[n], rsem.at[idx], layer=jnp.int32(t)))

    def lazy_sends(act):
        for i, t in tops:
            low = coarse[i - 1] if i else 0

            @pl.when(layer == t)
            def _():
                for n, target in enumerate(range(low, t)):
                    act(send(err_bf, err_in, s_lz.at[n], r_lz.at[0], layer=jnp.int32(target)))

    for load in small[1:3]:
        load.wait()
    pl.semaphore_wait(barrier, layers - 1 + dpn - 1)
    start = lambda c: c.start()

    @pl.when(layer > 0)
    def _():
        for r in range(cuts):
            up_guess(r).start()

    coarse_sends(rate_ref, crate, s_cr, r_cr, start, True)
    small[0].wait()
    to_mate = lambda i, src, dst: send(src, dst, s_mate.at[i], r_mate.at[i], dp=mate)
    mate_x = lambda: to_mate(0, x_ref, x_far)
    mate_ctx = lambda: to_mate(1, ctx, ctx_far)
    mate_d2 = lambda r: to_mate(2 + r, d2_bf.at[span(r)], d2_far.at[span(r)])
    if paired:
        mate_x().start()
    loads[0].wait()
    qkv[...] = nn(x_ref[...], wqkv[...]).astype(BF)
    q_t[...] = qkv[:, :width].T
    for s in range(sentences):
        rows = pl.ds(s * SEQ, SEQ)
        row_at = lax.broadcasted_iota(jnp.int32, (SEQ, SEQ), 0)
        col_at = lax.broadcasted_iota(jnp.int32, (SEQ, SEQ), 1)
        bias[...] = jnp.where((col_at <= row_at) & (col_at < len_ref[s]), 0.0, -1e30)

        def attend(i):
            lanes = lambda k: pl.ds(k * width + i * 128, 128)
            q, k, v = qkv[rows, lanes(0)], qkv[rows, lanes(1)], qkv[rows, lanes(2)]
            outs = []
            for h in range(2):
                cut = slice(h * HEAD_DIM, (h + 1) * HEAD_DIM)
                sc = nt(q[:, cut], k[:, cut]) * scale + bias[...]
                e = jnp.exp(sc - jnp.max(sc, axis=-1, keepdims=True))
                p = e * (1.0 / jnp.sum(e, axis=-1, keepdims=True))
                probs[s, 2 * i + h] = p
                outs.append(nn(p.astype(BF), v[:, cut]))
            ctx[rows, lanes(0)] = jnp.concatenate(outs, axis=-1).astype(BF)

        for i in range(pairs):
            attend(i)
    coarse_sends(guess_ref, cguess, s_cg, r_cg, start, False)
    if paired:
        mate_ctx().start()
    for load in small[3:]:
        load.wait()
    gain1, gain2 = gain1_ref[...], gain2_ref[...]
    loads[1].wait()
    u, iv = unit_of(DEPTH_GAIN * x_ref[...].astype(F32) + nn(ctx[...], wout[...]))
    unit1[...] = u
    inv1[...] = iv
    normed_bf[...] = (u * gain1).astype(BF)
    loads[2].wait()
    step = 512

    def feed_forward(normed, out, slope):
        def feed(i):
            lanes = pl.ds(i * step, step)
            pre = nn(normed[...], win[:, lanes])
            sq = pre * pre
            t = jnp.tanh(TANH_SCALE * (pre + CUBIC * sq * pre))
            out[:, lanes] = (0.5 * pre * (1.0 + t)).astype(BF)
            slope[:, lanes] = 0.5 * (1.0 + t) + 0.5 * pre * (1.0 - t * t) * TANH_SCALE * (
                1.0 + 3.0 * CUBIC * sq
            )

        with jax.named_scope("feed"):
            for i in range(hidden_units // step):
                feed(i)

    feed_forward(normed_bf, hidden, deriv)
    loads[3].wait()
    u, iv = unit_of(DEPTH_GAIN * (unit1[...] * gain1) + nn(hidden[...], wback[...]))
    unit2[...] = u
    inv2[...] = iv

    grads = (
        (part_back, r1_back, r2_back, gback_ref),
        (part_in, r1_in, r2_in, gin_ref),
        (part_out, r1_out, r2_out, gout_ref),
        (part_qkv, r1_qkv, r2_qkv, gqkv_ref),
    )

    def near(g, i):
        part, r1, _, _ = grads[g]
        size = r1.shape[1]
        at = pl.multiple_of((2 * i + 1 - core) * size, size)
        return send(
            part.at[pl.ds(at, size)], r1.at[i], s1.at[g, i], q1.at[g, i],
            dp=2 * chip + 1 - core,
        )

    def far(g, o):
        _, r1, r2, _ = grads[g]
        i = lax.rem(chip + o, chips)
        return send(
            r1.at[i], r2.at[o - 1], s2.at[g, o - 1], q2.at[g, o - 1], dp=2 * i + core
        )

    def mine(g, i):
        part, r1, _, _ = grads[g]
        size = r1.shape[1]
        return part[pl.ds(pl.multiple_of((2 * i + core) * size, size), size)].astype(F32)

    def to_partner(g):
        for i in range(chips):
            near(g, i).start()

    def to_chips(g):
        r1 = grads[g][1]
        for i in range(chips):
            near(g, i).wait_recv()
        for o in range(1, chips):
            i = lax.rem(chip + o, chips)
            r1[i] = (r1[i].astype(F32) + mine(g, i)).astype(BF)
            far(g, o).start()

    def finish(g):
        _, r1, r2, out = grads[g]
        total = r1[chip].astype(F32) + mine(g, chip)
        for o in range(1, chips):
            far(g, o).wait_recv()
            total = total + r2[o - 1].astype(F32)
        out[...] = total.astype(out.dtype)

    def transposed(left, right, out):
        cols = min(step, left.shape[1])

        def body(i, carry):
            at = pl.ds(pl.multiple_of(i * cols, cols), cols)
            out[at, :] = tn(left[:, at], right).astype(BF)
            return carry

        lax.fori_loop(0, left.shape[1] // cols, body, 0)

    def hidden_back(d, slope, out):
        with jax.named_scope("du"):
            for i in range(hidden_units // step):
                lanes = pl.ds(i * step, step)
                out[:, lanes] = (nt(d[...], wback[lanes, :]) * slope[:, lanes]).astype(BF)

    def to_second(r, final):
        at = span(r)
        d2, grad_two = norm_back(up_bf[at, :].astype(F32), unit2[at, :], inv2[at, :], gain2)
        d2_bf[at, :] = d2.astype(BF)
        if final and paired:
            mate_d2(r).start()
        dfirst[at, :] = DEPTH_GAIN * d2
        if final:
            gsum[1:2, :] = grad_two if r == 0 else gsum[1:2, :] + grad_two

    def to_scores(final):
        hidden_back(d2_bf, deriv, dpre)
        dn = dfirst[...] + nt(dpre[...], win[...])
        d1, grad_one = norm_back(dn, unit1[...], inv1[...], gain1)
        dfirst[...] = DEPTH_GAIN * d1
        up_bf[...] = d1.astype(BF)
        if final:
            gsum[0:1, :] = grad_one
        dctx[...] = nt(up_bf[...], wout[...]).astype(BF)
        dctx_t[...] = dctx[...].T

    def to_state(out):
        with jax.named_scope("dstate"):
            out[...] = (dfirst[...] + nt(dqkv[...], wqkv[...])).astype(BF)

    def attend_back(s, i):
        rows = pl.ds(s * SEQ, SEQ)
        lanes = lambda k: pl.ds(k * width + i * 128, 128)
        k, v = qkv[rows, lanes(1)], qkv[rows, lanes(2)]
        dc = dctx[rows, lanes(0)]
        outs = ([], [], [])
        for h in range(2):
            cut = slice(h * HEAD_DIM, (h + 1) * HEAD_DIM)
            own = pl.ds(i * 128 + h * HEAD_DIM, HEAD_DIM)
            p = probs[s, 2 * i + h]
            dp_ = nt(dc[:, cut], v[:, cut])
            outs[2].append(nn(dctx_t[own, rows], p.astype(BF)))
            ds = p * (dp_ - jnp.sum(p * dp_, axis=-1, keepdims=True)) * scale
            ds = ds.astype(BF)
            outs[0].append(nn(ds, k[:, cut]))
            outs[1].append(nn(q_t[own, rows], ds))
        dqkv[rows, lanes(0)] = jnp.concatenate(outs[0], axis=-1).astype(BF)
        for n in (1, 2):
            dqkv[rows, lanes(n)] = jnp.concatenate(outs[n], axis=0).astype(BF).T

    def attention_back():
        with jax.named_scope("att2"):
            for s in range(sentences):
                for i in range(pairs):
                    attend_back(s, i)

    def backward_summed():
        transposed(hidden, d2_bf[...], part_back)
        to_partner(0)
        transposed(normed_bf, dpre[...], part_in)
        to_partner(1)
        to_chips(0)
        transposed(ctx, up_bf[...], part_out)
        to_partner(2)
        to_chips(1)
        attention_back()
        to_chips(2)
        transposed(x_ref, dqkv[...], part_qkv)
        to_partner(3)
        to_state(adj_ref)

    def half_send(g):
        src, dst = ((half_s, half_r), (quarter_s, quarter_r), (small_s, small_r))[g]
        return send(src, dst, s_half.at[g], r_half.at[g], dp=sibling)

    def near_qkv(i, c):
        size = pq.shape[1] // dpn
        at = pl.multiple_of((2 * c + 1 - core) * size, size)
        return send(
            pq.at[i, pl.ds(at, size)], pq1.at[i, c], sq1.at[i, c], rq1.at[i, c], dp=sibling
        )

    def mine_qkv(i, c):
        size = pq.shape[1] // dpn
        at = pl.multiple_of((2 * c + core) * size, size)
        return pq[i, pl.ds(at, size)].astype(F32)

    def far_qkv(i):
        return send(pq1.at[i, 1 - chip], pq2.at[i], sq2.at[i], rq2.at[i], dp=mate)

    def relay_qkv(i):
        near_qkv(i, 1 - chip).wait_recv()
        pq1[i, 1 - chip] = (pq1[i, 1 - chip].astype(F32) + mine_qkv(i, 1 - chip)).astype(BF)
        far_qkv(i).start()

    def finish_qkv(i):
        near_qkv(i, chip).wait_recv()
        total = pq1[i, chip].astype(F32) + mine_qkv(i, chip)
        far_qkv(i).wait_recv()
        total = total + pq2[i].astype(F32)
        for n in range(3):
            gqkv_ref[:, n * width + i * 128 : n * width + (i + 1) * 128] = total[
                :, n * 128 : (n + 1) * 128
            ]

    def rows_of(left, left_far, right, right_far, c, size):
        at = pl.ds(pl.multiple_of((2 * chip + c) * size, size), size)
        return tn(left[:, at], right[...]) + tn(left_far[:, at], right_far[...])

    def look_ahead():
        mate_x().wait_recv()
        mate_ctx().wait_recv()
        u, iv = unit_of(DEPTH_GAIN * x_far[...].astype(F32) + nn(ctx_far[...], wout[...]))
        unit1_far[...] = u
        inv1_far[...] = iv
        normed_far[...] = (u * gain1).astype(BF)
        feed_forward(normed_far, hidden_far, deriv_far)
        x_t[...] = x_ref[...].T

    def backward_paired():
        for i in range(pairs):
            with jax.named_scope("att2"):
                for s in range(sentences):
                    attend_back(s, i)
            with jax.named_scope("gqkv"):
                cut = [dqkv[:, n * width + i * 128 : n * width + (i + 1) * 128] for n in range(3)]
                pq[i] = nn(x_t[...], jnp.concatenate(cut, axis=-1)).astype(BF)
                near_qkv(i, 1 - chip).start()
                near_qkv(i, chip).start()
            if i:
                relay_qkv(i - 1)
        with jax.named_scope("wd2"):
            for r in range(cuts):
                mate_d2(r).wait_recv()
        hidden_back(d2_far, deriv_far, dpre_far)
        relay_qkv(pairs - 1)
        d2o = d2_far[...].astype(F32)
        d1, _ = norm_back(
            DEPTH_GAIN * d2o + nt(dpre_far[...], win[...]), unit1_far[...], inv1_far[...], gain1
        )
        d1_far[...] = d1.astype(BF)
        parts = (
            (hidden, hidden_far, d2_bf, d2_far, half_s, gback_ref),
            (normed_bf, normed_far, dpre, dpre_far, quarter_s, gin_ref),
            (ctx, ctx_far, up_bf, d1_far, small_s, gout_ref),
        )
        with jax.named_scope("gpart"):
            for g, (a, a_far, b, b_far, out, _) in enumerate(parts):
                out[...] = rows_of(a, a_far, b, b_far, 1 - core, out.shape[0]).astype(BF)
                half_send(g).start()
            for a, a_far, b, b_far, _, out in parts:
                out[...] = rows_of(a, a_far, b, b_far, core, out.shape[0])
        to_state(adj_ref)

    def gain_send(o):
        return send(
            gsum, grecv.at[o - 1], s_g.at[o - 1], r_g.at[o - 1], dp=lax.rem(dp + o, dpn)
        )

    for r in range(cuts):

        @pl.when(is_last)
        def _():
            up_bf[span(r), :] = cot_ref[span(r), :]

        @pl.when(layer < last)
        def _():
            up_guess(r).wait_recv()
            up_bf[span(r), :] = above[span(r), :]

        to_second(r, False)

    to_scores(False)

    attention_back()
    plain_sender = (layer > 0) & jnp.logical_not(is_coarse)
    to_state(relaxed)
    for r in range(cuts):

        @pl.when(plain_sender)
        def _():
            up_relaxed(r).start()

        crel_sends(r, start)
    if paired:
        look_ahead()

    def build_err(r):
        at = span(r)
        here = jnp.int32(0)
        for i, t in tops:

            @pl.when(layer == t)
            def _():
                for idx in reversed(range(i, len(coarse))):
                    if r == 0:
                        send(rate_ref, crate.at[idx], s_cr.at[0], r_cr.at[idx], layer=here).wait_recv()
                        if idx > i:
                            send(guess_ref, cguess.at[idx], s_cg.at[0], r_cg.at[idx], layer=here).wait_recv()
                    crel_send(idx, 0, r, here).wait_recv()
                    old = above[at, :] if idx == i else cguess[idx, at, :]
                    resid = crel[idx, at, :].astype(F32) - old.astype(F32)
                    above_it = idx < len(coarse) - 1
                    err[at, :] = crate[idx] * err[at, :] + resid if above_it else resid

        err_bf[at, :] = err[at, :].astype(BF)

    for r in range(cuts):

        @pl.when(is_last)
        def _():
            up_bf[span(r), :] = cot_ref[span(r), :]

        @pl.when(next_plain)
        def _():
            with jax.named_scope("wrel"):
                up_relaxed(r).wait_recv()
            up_bf[span(r), :] = above2[span(r), :]

        @pl.when(next_coarse)
        def _():
            with jax.named_scope("werr"):
                build_err(r)
            up_bf[span(r), :] = (above[span(r), :].astype(F32) + err[span(r), :]).astype(BF)

        to_second(r, True)

    to_scores(True)

    for o in range(1, dpn):
        gain_send(o).start()

    @pl.when(next_coarse)
    def _():
        lazy_sends(start)

    if paired:
        backward_paired()
    else:
        backward_summed()
        to_chips(3)

    @pl.when(is_last)
    def _():
        err[...] = jnp.zeros_like(err)

    @pl.when(next_plain)
    def _():
        send(err_bf, err_in, s_lz.at[0], r_lz.at[0], layer=jnp.int32(0)).wait_recv()
        err[...] = err_in[...].astype(F32)

    @pl.when(is_coarse)
    def _():
        own = guess_ref[...].astype(F32)
        err[...] = rate_ref[...] * err[...] + (relaxed[...].astype(F32) - own)
        adj_ref[...] = (own + err[...]).astype(BF)

    err_ref[...] = err[...]
    if not paired:
        finish(0)
        finish(1)
    gains = gsum[...]
    for o in range(1, dpn):
        gain_send(o).wait_recv()
        gains = gains + grecv[o - 1]
    piece = width // dpn
    one, two = jnp.zeros((1, piece), F32), jnp.zeros((1, piece), F32)
    for c in range(dpn):
        cut = slice(c * piece, (c + 1) * piece)
        here = dp == c
        one = one + jnp.where(here, gains[0:1, cut], 0.0)
        two = two + jnp.where(here, gains[1:2, cut], 0.0)
    g1_ref[...] = one
    g2_ref[...] = two
    if paired:
        for g, (part, out) in enumerate(
            ((half_r, gback_ref), (quarter_r, gin_ref), (small_r, gout_ref))
        ):
            half_send(g).wait_recv()
            out[...] = out[...] + part[...].astype(F32)
        with jax.named_scope("finq"):
            for i in range(pairs):
                finish_qkv(i)
    else:
        finish(2)
        finish(3)

    sent = lambda c: c.wait_send()

    @pl.when(layer > 0)
    def _():
        for r in range(cuts):
            sent(up_guess(r))

    @pl.when(plain_sender)
    def _():
        for r in range(cuts):
            sent(up_relaxed(r))

    for r in range(cuts):
        crel_sends(r, sent)
    coarse_sends(guess_ref, cguess, s_cg, r_cg, sent, False)
    coarse_sends(rate_ref, crate, s_cr, r_cr, sent, True)
    lazy_sends(sent)
    if paired:
        for copy in [mate_x(), mate_ctx()] + [mate_d2(r) for r in range(cuts)]:
            sent(copy)
        for g in range(3):
            sent(half_send(g))
        for i in range(pairs):
            sent(near_qkv(i, 0))
            sent(near_qkv(i, 1))
            sent(far_qkv(i))
    else:
        for g in range(4):
            for i in range(chips):
                sent(near(g, i))
            for o in range(1, chips):
                sent(far(g, o))
    for o in range(1, dpn):
        sent(gain_send(o))


def writer(*refs):
    n = len(refs) // 2
    sems = refs[-1]
    copies = [
        pltpu.make_async_copy(refs[i], refs[n + i].at[0] if len(refs[n + i].shape) == 3 else refs[n + i], sems.at[i])
        for i in range(n)
    ]
    for copy in copies:
        copy.start()
    for copy in copies:
        copy.wait()


def on_device(layers, dpn, *args):
    (states, guess, cotangent, lengths, rate, w_qkv, w_out, w_in, w_back, gain1, gain2) = args
    tokens, width = states.shape[1:]
    ff = w_in.shape[2]
    heads = width // HEAD_DIM
    coarse = [j for j in range(1, layers) if j % FACTOR == 0 or j == layers - 1]
    n = len(coarse)
    chips = dpn // 2
    cuts = 2 if tokens % 256 == 0 else 1
    shapes = ((ff, width), (width, ff), (width, width), (width, 3 * width))
    vm = pltpu.VMEM
    rows = (tokens, width)
    dma = lambda *s: pltpu.SemaphoreType.DMA(s)
    line = vm((1, width), F32)
    scratch = [
        vm(rows, BF), vm(rows, BF), vm(rows, BF),
        line, line, line,
        vm((width, 3 * width), BF), vm((width, width), BF), vm((width, ff), BF),
        vm((ff, width), BF),
        vm((tokens, 3 * width), BF), vm((SEQ, SEQ), F32),
        vm((tokens // SEQ, heads, SEQ, SEQ), F32), vm(rows, BF), vm(rows, F32), vm(rows, F32),
        vm((tokens, 1), F32), vm((tokens, 1), F32), vm(rows, BF), vm((tokens, ff), BF),
        vm((tokens, ff), F32),
        vm(rows, BF), vm(rows, BF), vm((tokens, 3 * width), BF), vm((tokens, ff), BF),
        vm(rows, F32), vm(rows, BF),
        vm(rows, BF), vm(rows, BF), vm((n,) + rows, BF), vm((n,) + rows, BF),
        vm((n, 1, width), F32), vm(rows, F32), vm(rows, BF), vm(rows, BF),
    ]
    paired = chips == 2
    pairs = width // 128
    far = max(chips - 1, 1)
    tile = (8, 128)
    either = lambda use, s, t=BF: vm(s if use else tile, t)
    scratch += [either(not paired, s) for s in shapes]
    scratch += [either(not paired, (chips, s[0] // dpn, s[1])) for s in shapes]
    scratch += [either(not paired, (far, s[0] // dpn, s[1])) for s in shapes]
    scratch += [vm((2, width), F32), vm((dpn - 1, 2, width), F32)]
    scratch += [either(paired, rows) for _ in range(5)]
    scratch += [
        either(paired, (tokens, ff)), vm(rows, BF), either(paired, rows, F32),
        either(paired, (tokens, 1), F32), either(paired, (tokens, ff)),
        either(paired, (tokens, ff), F32), either(paired, (width, tokens)),
    ]
    for s in (shapes[0], shapes[1], shapes[2]):
        scratch += [either(paired, (s[0] // dpn, s[1])) for _ in range(2)]
    scratch += [
        either(paired, (pairs, width, 384)), either(paired, (pairs, 2, width // dpn, 384)),
        either(paired, (pairs, width // dpn, 384)), vm((width, tokens), BF), vm((width, tokens), BF),
    ]
    scratch += [
        dma(4), dma(6), dma(2, cuts), dma(2, cuts), dma(n), dma(n), dma(n), dma(n),
        dma(n, cuts), dma(n, cuts),
        dma(FACTOR), dma(1),
        dma(4, chips), dma(4, chips), dma(4, far), dma(4, far), dma(dpn - 1), dma(dpn - 1),
        dma(2 + cuts), dma(2 + cuts), dma(3), dma(3), dma(pairs, 2), dma(pairs, 2), dma(pairs), dma(pairs),
    ]
    left = pl.BlockSpec(memory_space=pltpu.HBM)
    whole = pl.BlockSpec(memory_space=pltpu.VMEM)
    piece = lambda s: vm((s[0] // dpn, s[1]), F32)
    small = vm((1, width // dpn), F32)
    results = pl.pallas_call(
        functools.partial(kernel, layers, dpn, coarse, cuts),
        out_shape=(
            vm(rows, BF), vm(rows, F32), piece(shapes[3]), piece(shapes[2]), piece(shapes[1]),
            piece(shapes[0]), small, small,
        ),
        in_specs=[pl.BlockSpec(memory_space=pltpu.SMEM)] + [left] * 10,
        out_specs=(whole,) * 8,
        scratch_shapes=scratch,
        compiler_params=pltpu.CompilerParams(
            collective_id=0, has_side_effects=True, vmem_limit_bytes=48 * 1024 * 1024
        ),
    )(
        lengths,
        *(
            pltpu.with_memory_space_constraint(a, pltpu.HBM)
            for a in (
                states[0], guess[0], cotangent, rate, gain1, gain2,
                w_qkv[0], w_out[0], w_in[0], w_back[0],
            )
        )
    )
    results = [pltpu.with_memory_space_constraint(r, pltpu.VMEM) for r in results]
    shape = lambda r: r.shape if r.shape[0] == 1 else (1,) + r.shape
    return pl.pallas_call(
        writer,
        out_shape=tuple(jax.ShapeDtypeStruct(shape(r), r.dtype) for r in results),
        in_specs=[whole] * 8,
        out_specs=(left,) * 8,
        scratch_shapes=[dma(8)],
        compiler_params=pltpu.CompilerParams(vmem_limit_bytes=1024 * 1024),
    )(*results)


def solution(mesh):
    placed = (
        P("layer", "dp", None), P("layer", "dp", None), P("dp", None), P("dp"),
        P("layer", None), P("layer", None, None), P("layer", None, None),
        P("layer", None, None), P("layer", None, None), P("layer", None), P("layer", None),
    )
    split = P("layer", "dp", None)
    return jax.shard_map(
        functools.partial(on_device, mesh.shape["layer"], mesh.shape["dp"]),
        mesh=mesh,
        in_specs=placed,
        out_specs=(split,) * 6 + (P("layer", "dp"),) * 2,
        check_vma=False,
    )
```
